32 devices in a mesh: rows: 4 (over y, x), cols: 2 (over core), reps: 4 (over z).
Axes of the slice: x: 2, y: 2, z: 4, core: 2. Of those that a mesh axis runs over, the one named last changes fastest.
Arguments:
- features: bfloat16 [4096, 512], P('rows', 'cols'), may hold values from -6 to 6
- tiles: bfloat16 [1024, 128, 128], P(('rows', 'reps')), may hold values from -0.1875 to 0.1875
- tile_cols: int32 [16, 64], P(('rows', 'reps')), may hold values from 0 to 31, as said below
- tile_ptr: int32 [16, 9], P(('rows', 'reps')), may hold values from 0 to 64, as said below
Outputs:
- aggregated: bfloat16 [4096, 512], P(('rows', 'reps'), 'cols')
The draws below stay inside these ranges and needn't reach their ends.
Inputs may be any that keep to these rules, and one draw needn't show every extreme that they name: `tile_cols`: slot j of row g = b * 4 + q with key k (see steps) lies in section s = k // 8; its column tile is c * 8 + e with column block c = (b + q * 1 + s) mod 4 and 0 <= e < 8. Live slots name distinct tiles and are in order of key. Slots that are not live hold 0 and arbitrary tile values. `tile_ptr`: each row starts at 0 and never falls; its last entry, the live count, is at least 1 and equals 64 on some row of every draw; counts are skewed, most rows holding a quarter of 64 or less.
All inputs are finite; a program needn't handle non-finite values.
Results may differ from the reference program's by a relative error of at most 0.001.
Values may be sent and summed in bfloat16 or wider, within the bound.
A program may use at most 64 MiB of HBM per device.

```python
import jax
import jax.numpy as jnp
from jax import lax

TILE = 128
FEAT = 512
TB = 8
SECTIONS = 1
SLOTS = 64
NODES = 4096
N_ROWS = 4
N_REPS = 4


def tile_layout(key):
    base = jax.random.fold_in(key, 11)
    key_a, key_b, key_c, key_d = jax.random.split(base, 4)
    num_devices = N_ROWS * N_REPS
    level_a = jax.random.randint(key_a, (num_devices,), 0, 4)
    level_b = jax.random.randint(key_b, (num_devices,), 0, 4)
    levels = jnp.maximum(level_a, level_b).astype(jnp.int32)
    counts = jnp.right_shift(jnp.full((num_devices,), SLOTS, jnp.int32), levels)
    counts = jnp.maximum(counts, 1)
    fullest = jax.random.randint(key_c, (), 0, num_devices)
    device_ids = jnp.arange(num_devices, dtype=jnp.int32)
    counts = jnp.where(device_ids == fullest, SLOTS, counts).astype(jnp.int32)

    def shuffled(sub_key):
        return jax.random.permutation(sub_key, SLOTS)
    orders = jax.vmap(shuffled)(jax.random.split(key_d, num_devices))
    ranks = jnp.argsort(orders, axis=1).astype(jnp.int32)
    chosen = ranks < counts[:, None]
    positions = jnp.argsort(1 - chosen.astype(jnp.int32), axis=1, stable=True).astype(jnp.int32)
    valid = jnp.arange(SLOTS, dtype=jnp.int32)[None, :] < counts[:, None]
    section_of = positions // (TB * TB)
    within = positions % TB
    row_block = device_ids // N_REPS
    replica = device_ids % N_REPS
    col_block = (row_block[:, None] + replica[:, None] * SECTIONS + section_of) % N_ROWS
    col_ids = jnp.where(valid, col_block * TB + within, 0).astype(jnp.int32)
    pos_keys = jnp.arange(SLOTS, dtype=jnp.int32) // TB
    marks = jnp.arange(SECTIONS * TB + 1, dtype=jnp.int32)
    pointers = jnp.sum((chosen[:, None, :] & (pos_keys[None, None, :] < marks[None, :, None])).astype(jnp.int32), axis=2)
    return (col_ids, pointers.astype(jnp.int32))


def draw_tile_cols(key, part):
    return tile_layout(key)[0]


def draw_tile_ptr(key, part):
    return tile_layout(key)[1]


def shard_levels(rng, extent, cuts, least, largest):
    def one(axis_at, shards_of):
        draws = jax.random.uniform(jax.random.fold_in(jax.random.fold_in(rng, 6), axis_at), (shards_of,), jnp.float32, least / len(cuts), largest / len(cuts))
        return jnp.repeat(jnp.exp(draws), extent[axis_at] // shards_of).reshape((-1,) + (1,) * (len(extent) - axis_at - 1))

    loudness = one(*cuts[0])
    for cut in cuts[1:]:
        loudness = loudness * one(*cut)
    return loudness


def scatter_about(own_key, shape, scale, reach, shards=(), kind=jnp.bfloat16):
    values = scale * jax.random.normal(own_key, shape, jnp.float32)
    if shards:
        values = values * shard_levels(own_key, shape, shards, -0.22, 0.18)
    return jnp.clip(values, -reach, reach).astype(kind)


def setup_inputs(seed: int = 0) -> dict:
    keys = jax.random.split(jax.random.key(seed), 5)
    features = scatter_about(keys[0], (NODES, FEAT), 1.0, 6.0, ((0, 4), (1, 2)))
    tiles = scatter_about(keys[1], (N_ROWS * N_REPS * SLOTS, TILE, TILE), (TILE * TB) ** -0.5, 0.1875, ((0, 16),))
    tile_cols = draw_tile_cols(jax.random.fold_in(keys[4], 71), 0)
    tile_ptr = draw_tile_ptr(jax.random.fold_in(keys[4], 71), 0)
    return dict(features=features, tiles=tiles, tile_cols=tile_cols, tile_ptr=tile_ptr)


def slot_rows(pointers, num_slots):
    slot_ids = jnp.arange(num_slots, dtype=jnp.int32)
    slot_keys = jnp.sum((pointers[None, 1:] <= slot_ids[:, None]).astype(jnp.int32), axis=1)
    return (slot_keys % TB).astype(jnp.int32)


def reference(features, tiles, tile_cols, tile_ptr):
    num_slots = tile_cols.shape[1]
    feat_tiles = features.reshape(N_ROWS * TB, TILE, FEAT)
    dev_tiles = tiles.reshape(N_ROWS * N_REPS, num_slots, TILE, TILE)
    row_range = jnp.arange(TB, dtype=jnp.int32)

    def per_row_block(row_block):
        def one_device(replica, totals):
            device_num = (row_block * N_REPS + replica).astype(jnp.int32)
            own_tiles = dev_tiles[device_num]
            col_ids = tile_cols[device_num]
            pointers = tile_ptr[device_num]
            live_count = pointers[-1]
            row_ids = slot_rows(pointers, num_slots)
            num_blocks = (live_count + TB - 1) // TB

            def advance(block_num, inner):
                begin_at = (block_num * TB).astype(jnp.int32)
                tile_block = lax.dynamic_slice_in_dim(own_tiles, begin_at, TB, 0).astype(jnp.float32)
                col_block = lax.dynamic_slice_in_dim(col_ids, begin_at, TB, 0)
                row_block_ids = lax.dynamic_slice_in_dim(row_ids, begin_at, TB, 0)
                slot_ids = begin_at + jnp.arange(TB, dtype=jnp.int32)
                active = slot_ids < live_count
                feat_block = jnp.take(feat_tiles, col_block, axis=0).astype(jnp.float32)
                products = jnp.einsum("bij,bjf->bif", tile_block, feat_block, precision=lax.Precision.HIGHEST)
                row_onehot = ((row_block_ids[:, None] == row_range[None, :]) & active[:, None]).astype(jnp.float32)
                return inner + jnp.einsum("bt,bif->tif", row_onehot, products, precision=lax.Precision.HIGHEST)

            empty = jnp.zeros((TB, TILE, FEAT), jnp.float32)
            return totals + lax.fori_loop(0, num_blocks, advance, empty)

        return lax.fori_loop(0, N_REPS, one_device, jnp.zeros((TB, TILE, FEAT), jnp.float32))

    sums = lax.map(per_row_block, jnp.arange(N_ROWS, dtype=jnp.int32))
    return sums.reshape(NODES, FEAT).astype(jnp.bfloat16)
```

```python
import functools

import jax
import jax.numpy as jnp
from jax import lax
from jax.experimental import pallas as pl
from jax.experimental.pallas import tpu as pltpu
from jax.sharding import PartitionSpec as P

MESH = pl.DeviceIdType.MESH
LANES = 128
STEPS = 32767.0


def kernel(
    dims,
    feats_hbm,
    tiles_hbm,
    cols_hbm,
    ptr_hbm,
    out_ref,
    cols_ref,
    ptr_ref,
    mine,
    theirs,
    tbuf,
    dense,
    own,
    code_out,
    code_in,
    scale_out,
    scale_in,
    feat_sem,
    tile_sem,
    index_sem,
    fsend,
    frecv,
    csend,
    crecv,
    ssend,
    srecv,
    reached,
):
    num_rows, num_reps, sections, tile_rows, tile, slots, chunks = dims
    b = lax.axis_index("rows")
    q = lax.axis_index("reps")
    block = tile_rows * tile
    share = block // num_reps
    share_tiles = share // tile

    feat_copies = []
    for n in range(chunks):
        copy = pltpu.make_async_copy(
            feats_hbm.at[:, pl.ds(n * LANES, LANES)], mine.at[n], feat_sem.at[n]
        )
        copy.start()
        feat_copies.append(copy)
    tile_copy = pltpu.make_async_copy(tiles_hbm, tbuf.at[pl.ds(0, slots)], tile_sem)
    tile_copy.start()
    cols_copy = pltpu.make_async_copy(cols_hbm, cols_ref, index_sem.at[0])
    cols_copy.start()
    ptr_copy = pltpu.make_async_copy(ptr_hbm, ptr_ref, index_sem.at[1])
    ptr_copy.start()

    barrier = pltpu.get_barrier_semaphore()
    for near, inside in ((q - 1, q > 0), (q + 1, q < num_reps - 1)):

        @pl.when(inside)
        def _(near=near):
            pl.semaphore_signal(barrier, inc=1, device_id={"reps": near}, device_id_type=MESH)

    for s in range(sections):
        source = lax.rem(b + q * sections + s, num_rows)

        def greet(source=source):
            pl.semaphore_signal(barrier, inc=1, device_id={"rows": source}, device_id_type=MESH)

        if s == 0:
            pl.when(q != 0)(greet)
        else:
            greet()
    lines = jnp.minimum(q, 1) + jnp.minimum(num_reps - 1 - q, 1)
    pl.semaphore_wait(barrier, lines + sections - 1 + jnp.minimum(q, 1))

    def feature_send(s, n):
        target = lax.rem(b + 2 * num_rows - q * sections - s, num_rows)
        return pltpu.make_async_remote_copy(
            src_ref=mine.at[n],
            dst_ref=theirs.at[s, n],
            send_sem=fsend.at[s, n],
            recv_sem=frecv.at[s, n],
            device_id={"rows": target},
            device_id_type=MESH,
        )

    for n in range(chunks):
        feat_copies[n].wait()
        for s in range(sections):
            if s == 0:

                @pl.when(q != 0)
                def _(n=n):
                    feature_send(0, n).start()

                @pl.when(q == 0)
                def _(n=n):
                    pltpu.make_async_copy(mine.at[n], theirs.at[0, n], frecv.at[0, n]).start()
            else:
                feature_send(s, n).start()

    tbuf[slots] = jnp.zeros((tile, tile), tbuf.dtype)
    tile_copy.wait()
    cols_copy.wait()
    ptr_copy.wait()

    for s in range(sections):

        def fill(r, carry, s=s):
            k = s * tile_rows + r
            low = ptr_ref[0, k]
            high = ptr_ref[0, k + 1]
            chosen = [jnp.int32(slots)] * tile_rows
            for i in range(tile_rows):
                j = low + i
                where_at = jnp.minimum(j, slots - 1)
                e = jnp.where(j < high, lax.rem(cols_ref[0, where_at], tile_rows), -1)
                chosen = [jnp.where(e == x, where_at, chosen[x]) for x in range(tile_rows)]
            at = pl.multiple_of(r * tile, tile)
            for x in range(tile_rows):
                dense[pl.ds(at, tile), pl.ds((s * tile_rows + x) * tile, tile)] = tbuf[chosen[x]]
            return carry

        lax.fori_loop(0, tile_rows, fill, 0)

    def code_send(d, n):
        return pltpu.make_async_remote_copy(
            src_ref=code_out.at[d - 1, n],
            dst_ref=code_in.at[d - 1, n],
            send_sem=csend.at[d - 1, n],
            recv_sem=crecv.at[d - 1, n],
            device_id={"reps": lax.rem(q + d, num_reps)},
            device_id_type=MESH,
        )

    def scale_send(d, n):
        return pltpu.make_async_remote_copy(
            src_ref=scale_out.at[d - 1, n],
            dst_ref=scale_in.at[d - 1, n],
            send_sem=ssend.at[d - 1, n],
            recv_sem=srecv.at[d - 1, n],
            device_id={"reps": lax.rem(q + d, num_reps)},
            device_id_type=MESH,
        )

    def product(target, n):
        rows = pl.ds(pl.multiple_of(target * share, share), share)
        total = None
        for s in range(sections):
            term = jnp.dot(
                dense[rows, pl.ds(s * block, block)],
                theirs[s, n],
                preferred_element_type=jnp.float32,
            )
            total = term if total is None else total + term
        return total

    for reach in range(2, num_reps):
        for way in (0, 1):
            place = q if way == 0 else num_reps - 1 - q
            ahead = q + 1 if way == 0 else q - 1

            @pl.when(jnp.logical_and(place >= reach - 1, place < num_reps - 1))
            def _(way=way, reach=reach, ahead=ahead):
                pl.semaphore_signal(
                    reached.at[way, reach - 2],
                    inc=1,
                    device_id={"reps": ahead},
                    device_id_type=MESH,
                )

        for way in (0, 1):
            place = q if way == 0 else num_reps - 1 - q

            @pl.when(place >= reach)
            def _(way=way, reach=reach):
                pl.semaphore_wait(reached.at[way, reach - 2], 1)

    order = sorted(range(1, num_reps), key=lambda d: -min(d, num_reps - d))
    for n in range(chunks):
        for s in range(sections):
            if s == 0:

                @pl.when(q != 0)
                def _(n=n):
                    feature_send(0, n).wait_recv()

                @pl.when(q == 0)
                def _(n=n):
                    pltpu.make_async_copy(mine.at[n], theirs.at[0, n], frecv.at[0, n]).wait()
            else:
                feature_send(s, n).wait_recv()
        previous = None
        for d in order:
            total = product(lax.rem(q + d, num_reps), n)
            for t in range(share_tiles):
                part = total[t * tile : (t + 1) * tile]
                peak = jnp.maximum(jnp.max(jnp.abs(part), axis=0, keepdims=True), 1e-30)
                code = jnp.round(part * (STEPS / peak)).astype(jnp.int32).astype(jnp.int16)
                code_out[d - 1, n, pl.ds(t * tile, tile), :] = code
                scale_out[d - 1, n, pl.ds(t, 1), :] = peak * (1.0 / STEPS)
            if previous is not None:
                code_send(previous, n).start()
                scale_send(previous, n).start()
            previous = d
        own[n] = product(q, n)
        code_send(previous, n).start()
        scale_send(previous, n).start()

    for n in range(chunks):
        for d in order:
            code_send(d, n).wait_recv()
            scale_send(d, n).wait_recv()
        for t in range(share_tiles):
            total = own[n, pl.ds(t * tile, tile), :]
            for d in range(1, num_reps):
                code = code_in[d - 1, n, pl.ds(t * tile, tile), :].astype(jnp.int32)
                scale = scale_in[d - 1, n, pl.ds(t, 1), :]
                total = total + code.astype(jnp.float32) * scale
            out_ref[pl.ds(t * tile, tile), pl.ds(n * LANES, LANES)] = total.astype(out_ref.dtype)

    for n in range(chunks):
        for s in range(sections):
            if s == 0:

                @pl.when(q != 0)
                def _(n=n):
                    feature_send(0, n).wait_send()
            else:
                feature_send(s, n).wait_send()
        for d in order:
            code_send(d, n).wait_send()
            scale_send(d, n).wait_send()


def body(features, tiles, tile_cols, tile_ptr):
    num_rows = lax.axis_size("rows")
    num_reps = lax.axis_size("reps")
    sections = num_rows // num_reps
    slots, tile = tiles.shape[0], tiles.shape[1]
    block, width = features.shape
    tile_rows = block // tile
    share = block // num_reps
    chunks = width // LANES
    share_tiles = share // tile
    dims = (num_rows, num_reps, sections, tile_rows, tile, slots, chunks)
    others = num_reps - 1
    dma = pltpu.SemaphoreType.DMA
    return pl.pallas_call(
        functools.partial(kernel, dims),
        out_shape=pltpu.VMEM((share, width), jnp.bfloat16),
        in_specs=[
            pl.BlockSpec(memory_space=pl.ANY),
            pl.BlockSpec(memory_space=pl.ANY),
            pl.BlockSpec(memory_space=pl.ANY),
            pl.BlockSpec(memory_space=pl.ANY),
        ],
        out_specs=pl.BlockSpec(memory_space=pltpu.VMEM),
        scratch_shapes=[
            pltpu.SMEM(tile_cols.shape, tile_cols.dtype),
            pltpu.SMEM(tile_ptr.shape, tile_ptr.dtype),
            pltpu.VMEM((chunks, block, LANES), features.dtype),
            pltpu.VMEM((sections, chunks, block, LANES), features.dtype),
            pltpu.VMEM((slots + 1, tile, tile), tiles.dtype),
            pltpu.VMEM((block, sections * block), tiles.dtype),
            pltpu.VMEM((chunks, share, LANES), jnp.float32),
            pltpu.VMEM((others, chunks, share, LANES), jnp.int16),
            pltpu.VMEM((others, chunks, share, LANES), jnp.int16),
            pltpu.VMEM((others, chunks, share_tiles, LANES), jnp.float32),
            pltpu.VMEM((others, chunks, share_tiles, LANES), jnp.float32),
            dma((chunks,)),
            dma,
            dma((2,)),
            dma((sections, chunks)),
            dma((sections, chunks)),
            dma((others, chunks)),
            dma((others, chunks)),
            dma((others, chunks)),
            dma((others, chunks)),
            pltpu.SemaphoreType.REGULAR((2, max(num_reps - 2, 1))),
        ],
        compiler_params=pltpu.CompilerParams(collective_id=0, has_side_effects=True),
        cost_estimate=pl.CostEstimate(
            flops=2 * block * block * sections * width, bytes_accessed=1 << 22, transcendentals=0
        ),
        name="graph_layer",
    )(features, tiles, tile_cols, tile_ptr)


def solution(mesh):
    placed = (
        P("rows", "cols"),
        P(("rows", "reps"), None, None),
        P(("rows", "reps"), None),
        P(("rows", "reps"), None),
    )
    return jax.shard_map(
        body, mesh=mesh, in_specs=placed, out_specs=P(("rows", "reps"), "cols"), check_vma=False
    )
```
